256 devices in a mesh: parts: 4 (over y, x), ka: 64 (over z, core).
Axes of the slice: x: 2, y: 2, z: 32, core: 2. Of those that a mesh axis runs over, the one named last changes fastest.
The devices are a block of a 4x8x32 slice.
Arguments:
- energies: float32 [256, 200], P(('parts', 'ka')), parts along dimension 0, may hold values from -4 to 4
- proj: float32 [256, 2, 10, 200], P(('parts', 'ka')), parts along dimension 0, may hold values from -0.3125 to 0.3125
- window: int32 [256, 2], P(('parts', 'ka')), parts along dimension 0, may hold values from 0 to 200, as said below
- sigma: float32 [8, 10, 10, 256], P('parts', None, None, 'ka'), parts along dimension 0, may hold values from -3 to 1.5, as said below
- impurity_inverse: float32 [8, 10, 10, 256], P('parts', None, None, 'ka'), parts along dimension 0, may hold values from -5 to 50, as said below
Outputs:
- density: float32 [256, 2, 200, 200], P(('parts', 'ka')), parts along dimension 0
- sigma_new: float32 [8, 10, 10, 256], P('parts', None, None, 'ka'), parts along dimension 0
The draws below stay inside these ranges and needn't reach their ends.
There are 4 independent parts, one for each index of `parts`. The reference program is written for one: setup_inputs(seed, part) draws one part's arguments, and reference() takes and returns one part's arrays. A program takes and returns all parts, laid end to end along the dimension named above; each array names one. Nothing has to cross between parts.
Inputs may be any that keep to these rules, and one draw needn't show every extreme that they name: window[k, 0] < 40 and window[k, 1] >= 160 for every k-point. For every frequency, sigma[0] and sigma[1] are real symmetric matrices and -sigma[1] is positive definite with smallest eigenvalue 0.2 or more. For every frequency n, impurity_inverse[0] and impurity_inverse[1] are real symmetric matrices and impurity_inverse[1] + sigma[1] - freqs[n] times the identity is positive definite with smallest eigenvalue 0.2 or more.
All inputs are finite; a program needn't handle non-finite values.
Results may differ from the reference program's by a relative error of at most 0.00011.
Values sent between devices are 32-bit elements; how exact they have to be, the bound alone decides.
A program may use at most 64 MiB of HBM per device.

```python
import math
import jax
import jax.numpy as jnp
from jax import lax

NORB = 10
NB = 200
NW = 256
K = 64


def draw_window(key, part):
    first = jax.random.randint(jax.random.fold_in(key, 11), (K,), 0, NB // 5)
    last = jax.random.randint(jax.random.fold_in(key, 12), (K,), NB - NB // 5, NB + 1)
    return jnp.stack([first, last], axis=1).astype(jnp.int32)


def sigma_parts(key):
    hermit = jnp.clip(0.5 * jax.random.normal(jax.random.fold_in(key, 21), (NORB, NORB, NW), jnp.float32), -1.5, 1.5)
    hermit = 0.5 * (hermit + jnp.swapaxes(hermit, 0, 1))
    damping = jnp.exp(jax.random.uniform(jax.random.fold_in(key, 22), (NORB, NW), jnp.float32, jnp.log(0.3), jnp.log(3.0)))
    offdiag = jax.random.uniform(jax.random.fold_in(key, 23), (NORB, NORB, NW), jnp.float32, -0.01, 0.01)
    ident = jnp.eye(NORB, dtype=jnp.float32)[:, :, None]
    offdiag = 0.5 * (offdiag + jnp.swapaxes(offdiag, 0, 1)) * (1.0 - ident)
    gamma = offdiag + ident * damping[:, None, :]
    return (hermit, gamma)


def draw_sigma(key, part):
    hermit, gamma = sigma_parts(key)
    return jnp.stack([hermit, -gamma]).astype(jnp.float32)


def draw_impurity_inverse(key, part):
    hermit, gamma = sigma_parts(key)
    level = jnp.clip(0.4 * jax.random.normal(jax.random.fold_in(key, 31), (NORB, NORB, NW), jnp.float32), -1.0, 1.0)
    level = 0.5 * (level + jnp.swapaxes(level, 0, 1))
    factor = jnp.clip(jax.random.normal(jax.random.fold_in(key, 32), (NORB, NORB, NW), jnp.float32), -3.0, 3.0)
    ident = jnp.eye(NORB, dtype=jnp.float32)[:, :, None]
    bath = 0.5 * jnp.einsum('ikn,jkn->ijn', factor, factor) / NORB + 0.2 * ident
    freqs = (2.0 * jnp.arange(NW).astype(jnp.float32) + 1.0) * (math.pi / 40.0)
    imag = ident * freqs[None, None, :] + bath + gamma
    return jnp.stack([level, imag]).astype(jnp.float32)


def steps_of(stream_key, dims, cuts, smallest, largest):
    def one(dim, parts):
        heights = jax.random.uniform(jax.random.fold_in(jax.random.fold_in(stream_key, 6), dim), (parts,), jnp.float32, smallest / len(cuts), largest / len(cuts))
        return jnp.repeat(jnp.exp(heights), dims[dim] // parts).reshape((-1,) + (1,) * (len(dims) - dim - 1))

    gain = one(*cuts[0])
    for cut in cuts[1:]:
        gain = gain * one(*cut)
    return gain


def noise(key, shape, deviation, most, pieces=(), held_as=jnp.bfloat16):
    gain = steps_of(key, shape, pieces, -0.22, 0.18) if pieces else 1.0
    entries = jax.random.normal(key, shape, jnp.float32) * deviation * gain
    return jnp.minimum(jnp.maximum(entries, -most), most).astype(held_as)


def setup_inputs(seed: int = 0, part: int = 0) -> dict:
    key_of = jax.random.split(jax.random.key(seed), 6)
    part_keys = jax.random.split(jax.random.fold_in(key_of[5], part), 6)
    return {
        "energies": jnp.clip(jax.random.uniform(part_keys[0], (K, NB), jnp.float32, -4.0, 4.0) * steps_of(part_keys[0], (K, NB), ((0, 64),), -0.4, 0.0), -4.0, 4.0),
        "proj": noise(part_keys[1], (K, 2, NORB, NB), (2 * NB) ** -0.5, 0.3125, ((0, 64),), jnp.float32),
        "window": draw_window(jax.random.fold_in(jax.random.fold_in(key_of[5], part), 71), part),
        "sigma": draw_sigma(jax.random.fold_in(jax.random.fold_in(key_of[5], part), 71), part),
        "impurity_inverse": draw_impurity_inverse(jax.random.fold_in(jax.random.fold_in(key_of[5], part), 71), part),
    }


highest = lax.Precision.HIGHEST
inverse_temp = 40.0


def matsubara(first, count):
    return (2.0 * (first + jnp.arange(count)).astype(jnp.float32) + 1.0) * (math.pi / inverse_temp)


def tail_weight(count):
    total = 0.0
    for number in range(count):
        total += (inverse_temp / (math.pi * (2 * number + 1))) ** 2
    return inverse_temp / 4.0 - 2.0 / inverse_temp * total


def propagators(energy, freqs):
    energy_b = energy[:, None, :]
    freq_b = freqs[None, :, None]
    denom = energy_b * energy_b + freq_b * freq_b
    return -energy_b / denom, -freq_b / denom


def hybrid(proj, green_re, green_im):
    proj_re = proj[:, 0]
    proj_im = proj[:, 1]
    left_re = proj_re[:, None] * green_re[:, :, None] - proj_im[:, None] * green_im[:, :, None]
    left_im = proj_re[:, None] * green_im[:, :, None] + proj_im[:, None] * green_re[:, :, None]
    hyb_re = jnp.einsum('kwib,kjb->ijkw', left_re, proj_re, precision=highest) + jnp.einsum('kwib,kjb->ijkw', left_im, proj_im, precision=highest)
    hyb_im = jnp.einsum('kwib,kjb->ijkw', left_im, proj_re, precision=highest) - jnp.einsum('kwib,kjb->ijkw', left_re, proj_im, precision=highest)
    return hyb_re, hyb_im


def invert(mat_re, mat_im):
    size = mat_re.shape[0]
    ident = jnp.eye(size, dtype=jnp.float32).reshape((size, size) + (1,) * (mat_re.ndim - 2)) * jnp.ones_like(mat_re)
    aug_re = jnp.concatenate([mat_re, ident], axis=1)
    aug_im = jnp.concatenate([mat_im, jnp.zeros_like(ident)], axis=1)
    for pivot in range(size):
        piv_re = aug_re[pivot, pivot]
        piv_im = aug_im[pivot, pivot]
        denom = piv_re * piv_re + piv_im * piv_im
        rec_re = piv_re / denom
        rec_im = -piv_im / denom
        row_re = aug_re[pivot] * rec_re - aug_im[pivot] * rec_im
        row_im = aug_re[pivot] * rec_im + aug_im[pivot] * rec_re
        col_re = aug_re[:, pivot][:, None]
        col_im = aug_im[:, pivot][:, None]
        next_re = aug_re - (col_re * row_re[None] - col_im * row_im[None])
        next_im = aug_im - (col_re * row_im[None] + col_im * row_re[None])
        aug_re = next_re.at[pivot].set(row_re)
        aug_im = next_im.at[pivot].set(row_im)
    return aug_re[:, size:], aug_im[:, size:]


def cmul(first_re, first_im, second_re, second_im):
    out_re = jnp.einsum('ij...,jk...->ik...', first_re, second_re, precision=highest) - jnp.einsum('ij...,jk...->ik...', first_im, second_im, precision=highest)
    out_im = jnp.einsum('ij...,jk...->ik...', first_re, second_im, precision=highest) + jnp.einsum('ij...,jk...->ik...', first_im, second_re, precision=highest)
    return out_re, out_im


def update_sigma(sig_re, sig_im, loc_re, loc_im, imp_re, imp_im):
    inv_re, inv_im = invert(loc_re, loc_im)
    diff_re = inv_re - imp_re
    diff_im = inv_im - imp_im
    new_re = sig_re + 0.5 * (diff_re + jnp.swapaxes(diff_re, 0, 1))
    new_im = sig_im + 0.5 * (diff_im - jnp.swapaxes(diff_im, 0, 1))
    return new_re, new_im


def dressed(ainv_re, ainv_im, sig_re, sig_im):
    return invert(ainv_re - sig_re[:, :, None, :], ainv_im - sig_im[:, :, None, :])


def vertex(sig_re, sig_im, gorb_re, gorb_im):
    wide_re = jnp.broadcast_to(sig_re[:, :, None, :], gorb_re.shape)
    wide_im = jnp.broadcast_to(sig_im[:, :, None, :], gorb_im.shape)
    half_re, half_im = cmul(wide_re, wide_im, gorb_re, gorb_im)
    full_re, full_im = cmul(half_re, half_im, wide_re, wide_im)
    return wide_re + full_re, wide_im + full_im


def band_density_total(proj, green_re, green_im, vertex_real, vert_im):
    proj_re = proj[:, 0]
    proj_im = proj[:, 1]
    wide_gre = green_re[:, :, None, :]
    wide_gim = green_im[:, :, None, :]
    left_re = wide_gre * proj_re[:, None] + wide_gim * proj_im[:, None]
    left_im = wide_gim * proj_re[:, None] - wide_gre * proj_im[:, None]
    mixed_re = jnp.einsum('ijkw,kjb->kwib', vertex_real, proj_re, precision=highest) - jnp.einsum('ijkw,kjb->kwib', vert_im, proj_im, precision=highest)
    mixed_im = jnp.einsum('ijkw,kjb->kwib', vertex_real, proj_im, precision=highest) + jnp.einsum('ijkw,kjb->kwib', vert_im, proj_re, precision=highest)
    right_re = mixed_re * wide_gre - mixed_im * wide_gim
    right_im = mixed_re * wide_gim + mixed_im * wide_gre
    real_total = jnp.einsum('kwib,kwic->kbc', left_re, right_re, precision=highest) - jnp.einsum('kwib,kwic->kbc', left_im, right_im, precision=highest)
    imaginary_total = jnp.einsum('kwib,kwic->kbc', left_re, right_im, precision=highest) + jnp.einsum('kwib,kwic->kbc', left_im, right_re, precision=highest)
    return real_total, imaginary_total


def limit_term(proj, herm_re, herm_im):
    proj_re = proj[:, 0]
    proj_im = proj[:, 1]
    hp_re = jnp.einsum('ij,kjc->kic', herm_re, proj_re, precision=highest) - jnp.einsum('ij,kjc->kic', herm_im, proj_im, precision=highest)
    hp_im = jnp.einsum('ij,kjc->kic', herm_re, proj_im, precision=highest) + jnp.einsum('ij,kjc->kic', herm_im, proj_re, precision=highest)
    quad_re = jnp.einsum('kib,kic->kbc', proj_re, hp_re, precision=highest) + jnp.einsum('kib,kic->kbc', proj_im, hp_im, precision=highest)
    quad_im = jnp.einsum('kib,kic->kbc', proj_re, hp_im, precision=highest) - jnp.einsum('kib,kic->kbc', proj_im, hp_re, precision=highest)
    return quad_re, quad_im


def high_part(new_re, new_im):
    last_re = new_re[:, :, -1]
    last_im = new_im[:, :, -1]
    return 0.5 * (last_re + last_re.T), 0.5 * (last_im - last_im.T)


def reference(energies, proj, window, sigma, impurity_inverse):
    band = jnp.arange(NB, dtype=jnp.int32)
    inside = ((band[None, :] >= window[:, 0:1]) & (band[None, :] < window[:, 1:2])).astype(jnp.float32)
    masked_values = proj * inside[:, None, None, :]
    freqs = matsubara(0, NW)
    green_re, green_im = propagators(energies, freqs)
    hyb_re, hyb_im = hybrid(masked_values, green_re, green_im)
    ainv_re, ainv_im = invert(hyb_re, hyb_im)
    gorb_re, gorb_im = dressed(ainv_re, ainv_im, sigma[0], sigma[1])
    loc_re = jnp.sum(gorb_re, axis=2) / K
    loc_im = jnp.sum(gorb_im, axis=2) / K
    new_re, new_im = update_sigma(sigma[0], sigma[1], loc_re, loc_im, impurity_inverse[0], impurity_inverse[1])
    gnew_re, gnew_im = dressed(ainv_re, ainv_im, new_re, new_im)
    vertex_real, vert_im = vertex(new_re, new_im, gnew_re, gnew_im)

    def one_point(entry_list):
        kpoint_projector, kpoint_green_real, kpoint_green_imag, kpoint_vertex_real, kpoint_vertex_imag = entry_list
        real_total, imaginary_total = band_density_total(kpoint_projector[None], kpoint_green_real[None], kpoint_green_imag[None], kpoint_vertex_real[:, :, None, :], kpoint_vertex_imag[:, :, None, :])
        return real_total[0], imaginary_total[0]

    real_total, imaginary_total = lax.map(one_point, (masked_values, green_re, green_im, jnp.moveaxis(vertex_real, 2, 0), jnp.moveaxis(vert_im, 2, 0)))
    herm_re, herm_im = high_part(new_re, new_im)
    quad_re, quad_im = limit_term(masked_values, herm_re, herm_im)
    weight = tail_weight(NW)
    dens_re = (real_total + jnp.swapaxes(real_total, 1, 2)) / inverse_temp - weight * quad_re
    dens_im = (imaginary_total - jnp.swapaxes(imaginary_total, 1, 2)) / inverse_temp - weight * quad_im
    density = jnp.stack([dens_re, dens_im], axis=1)
    sigma_new = jnp.stack([new_re, new_im])
    return density, sigma_new
```

```python
import math

import jax
import jax.numpy as jnp
from jax import lax
from jax.experimental import pallas as pl
from jax.experimental.pallas import tpu as pltpu
from jax.sharding import PartitionSpec as P

f32 = jnp.float32
bf16 = jnp.bfloat16
HI = lax.Precision.HIGHEST
MESH = pl.DeviceIdType.MESH
inverse_temp = 40.0
SEGS = 4
NO = 10
JP = 16
LN = 128


def tail_weight(count):
    total = 0.0
    for number in range(count):
        total += (inverse_temp / (math.pi * (2 * number + 1))) ** 2
    return inverse_temp / 4.0 - 2.0 / inverse_temp * total


def dot(a, b, ca, cb):
    return lax.dot_general(
        a, b, (((ca,), (cb,)), ((), ())), precision=HI, preferred_element_type=f32
    )


def bdot(a, b):
    return jnp.dot(a, b, preferred_element_type=f32)


def split(x):
    high = x.astype(bf16)
    return high, (x - high.astype(f32)).astype(bf16)


def iota(shape, dim):
    return lax.broadcasted_iota(jnp.int32, shape, dim)


def one_hot(cond):
    return jnp.where(cond, 1.0, 0.0).astype(f32)


def placed(array, line, p):
    pieces = [array[:p]] if p else []
    pieces.append(line)
    if p + 1 < array.shape[0]:
        pieces.append(array[p + 1 :])
    return jnp.concatenate(pieces, axis=0)


def invert(ar, ai):
    cols = iota(ar.shape, 1)
    for p in range(NO):
        pr, pi = ar[p : p + 1, p : p + 1, :], ai[p : p + 1, p : p + 1, :]
        inv = 1.0 / (pr * pr + pi * pi)
        rr, ri = pr * inv, -pi * inv
        rowr, rowi = ar[p : p + 1], ai[p : p + 1]
        at = cols[p : p + 1] == p
        nr = jnp.where(at, rr, rowr * rr - rowi * ri)
        ni = jnp.where(at, ri, rowr * ri + rowi * rr)
        cr, ci = ar[:, p : p + 1, :], ai[:, p : p + 1, :]
        br = jnp.where(cols == p, 0.0, ar)
        bi = jnp.where(cols == p, 0.0, ai)
        br = br - (cr * nr - ci * ni)
        bi = bi - (cr * ni + ci * nr)
        ar, ai = placed(br, nr, p), placed(bi, ni, p)
    return ar, ai


def cmul(ar, ai, br, bi):
    outr = outi = None
    for l in range(NO):
        xr, xi = ar[:, l : l + 1, :], ai[:, l : l + 1, :]
        yr, yi = br[l : l + 1], bi[l : l + 1]
        tr, ti = xr * yr - xi * yi, xr * yi + xi * yr
        outr = tr if outr is None else outr + tr
        outi = ti if outi is None else outi + ti
    return outr, outi


def build(devices, nf, bands):
    near = devices // SEGS
    own = SEGS * nf
    batch = near * own
    bp = (bands + LN - 1) // LN * LN
    rows = (bands + 15) // 16 * 16
    count = devices * nf
    step = near * nf
    per = 4
    groups = near // per
    gn = per * own
    weight = tail_weight(count)
    unit = math.pi / inverse_temp

    def freq_of(slot, place):
        return step * (slot // nf) + nf * place + slot % nf

    def kernel(
        w_ref, e_ref, proj_ref, sig_ref, imp_ref, dens_ref, out_ref,
        p16, pt, e2, sfix, s_all, part, send_a, recv_a, send_x, recv_x, h_src, h_dst,
        lh, ll, rh, rl, cacc,
        as_sem, ar_sem, xs_sem, xr_sem, ss_sem, sr_sem, ps_sem, pr_sem, hs_sem, hr_sem, loc_sem,
    ):
        me = lax.axis_index("ka")
        seg = me // near
        pos = lax.rem(me, near)
        base = seg * near
        up = lax.rem(me + near, devices)
        down = lax.rem(me + devices - near, devices)
        seg_up = lax.rem(seg + 1, SEGS)
        seg_down = lax.rem(seg + SEGS - 1, SEGS)
        seg_far = lax.rem(seg + 2, SEGS)

        def peer(off):
            return lax.rem(pos + off, near)

        barrier = pltpu.get_barrier_semaphore()
        for target in (up, down):
            pl.semaphore_signal(barrier, inc=1, device_id={"ka": target}, device_id_type=MESH)

        def greet(off, _):
            pl.semaphore_signal(
                barrier, inc=1, device_id={"ka": base + peer(off)}, device_id_type=MESH
            )
            return 0

        lax.fori_loop(1, near, greet, 0)

        lane = iota((1, bands), 1)
        inside = jnp.where((lane >= w_ref[0, 0]) & (lane < w_ref[0, 1]), 1.0, 0.0).astype(f32)
        p16[...] = jnp.zeros_like(p16)
        e2[...] = jnp.zeros_like(e2)
        e2[0:1, 0:bands] = e_ref[...]
        for c in range(2):
            for i in range(NO):
                p16[c, i : i + 1, 0:bands] = proj_ref[0, i, c : c + 1, :] * inside
        for kind, ref in enumerate((sig_ref, imp_ref)):
            for c in range(2):
                for i in range(NO):
                    at = 2 * nf * kind + nf * c
                    sfix[i, at : at + nf, :] = ref[c, i]
        packed = None
        for i in range(NO):
            place = one_hot(iota((NO, LN), 1) == NO * i + iota((NO, LN), 0))
            term = dot(sfix[i], place, 1, 0)
            packed = term if packed is None else packed + term
        s_all[seg] = packed

        oh_i = one_hot((iota((JP, LN), 1) // NO == iota((JP, LN), 0)) & (iota((JP, LN), 1) < NO * NO))
        oh_j = one_hot(
            (lax.rem(iota((JP, LN), 1), NO) == iota((JP, LN), 0)) & (iota((JP, LN), 1) < NO * NO)
        )
        pr, pi = p16[0], p16[1]
        pir, pii = dot(pr, oh_i, 0, 0), dot(pi, oh_i, 0, 0)
        pjr, pji = dot(pr, oh_j, 0, 0), dot(pi, oh_j, 0, 0)
        ppr = pir * pjr + pii * pji
        ppi = pii * pjr - pir * pji
        eye = one_hot(iota((JP, JP), 0) == iota((JP, JP), 1))
        pt[0] = dot(pr, eye, 0, 0)
        pt[1] = dot(pi, eye, 0, 0)

        row = iota((near * 2 * own, bp), 0)
        num = freq_of(lax.rem(row, own), row // (2 * own))
        omega = (2.0 * num.astype(f32) + 1.0) * unit
        energy = e2[0:1, :]
        recip = 1.0 / (energy * energy + omega * omega)
        g1, g2 = -energy * recip, -omega * recip
        real_row = lax.rem(row // own, 2) == 0
        a_all = dot(jnp.where(real_row, g1, g2), ppr, 1, 0) + dot(
            jnp.where(real_row, -g2, g1), ppi, 1, 0
        )
        send_a[...] = a_all.reshape(near, 2 * own, LN)

        pl.semaphore_wait(barrier, near + 1)

        def far_copy(buf, index, lo, size, sems, sem, target):
            return pltpu.make_async_remote_copy(
                src_ref=buf.at[index, pl.ds(lo, size), :],
                dst_ref=buf.at[index, pl.ds(lo, size), :],
                send_sem=sems[0].at[sem],
                recv_sem=sems[1].at[sem],
                device_id={"ka": target},
                device_id_type=MESH,
            )

        def far_start(buf, size, sems):
            far_copy(buf, seg, 0, size, sems, 0, up).start()
            far_copy(buf, seg, 0, size, sems, 1, down).start()

        def far_relay(buf, size, sems):
            half = size // 2
            far_copy(buf, seg_down, 0, size, sems, 0, up).wait_recv()
            far_copy(buf, seg_down, 0, half, sems, 2, up).start()
            far_copy(buf, seg_up, 0, size, sems, 1, down).wait_recv()
            far_copy(buf, seg_up, half, half, sems, 3, down).start()

        def far_end(buf, size, sems):
            half = size // 2
            far_copy(buf, seg_far, 0, half, sems, 2, up).wait_recv()
            far_copy(buf, seg_far, half, half, sems, 3, down).wait_recv()
            far_copy(buf, seg, 0, size, sems, 0, up).wait_send()
            far_copy(buf, seg, 0, size, sems, 1, down).wait_send()
            far_copy(buf, seg_down, 0, half, sems, 2, up).wait_send()
            far_copy(buf, seg_up, half, half, sems, 3, down).wait_send()

        def near_copy(src, dst, to, source, sems):
            return pltpu.make_async_remote_copy(
                src_ref=src.at[to],
                dst_ref=dst.at[source],
                send_sem=sems[0].at[to],
                recv_sem=sems[1].at[source],
                device_id={"ka": base + to},
                device_id_type=MESH,
            )

        order = [near // 2]
        for k in range(1, near // 2):
            order += [near // 2 - k, near // 2 + k]

        def near_start(src, dst, sems):
            for off in order:
                near_copy(src, dst, peer(off), pos, sems).start()

        s_sems, p_sems = (ss_sem, sr_sem), (ps_sem, pr_sem)
        a_sems, x_sems = (as_sem, ar_sem), (xs_sem, xr_sem)
        s_rows = 4 * nf
        far_start(s_all, s_rows, s_sems)
        near_start(send_a, recv_a, a_sems)
        recv_a[pos] = send_a[pos]

        e_col = dot(e2[0:1, :], jnp.ones((1, LN), f32), 0, 0)[0:rows]

        def left(g, _):
            ln = iota((rows, LN), 1)
            n64 = lax.rem(ln, gn)
            om = (
                2.0 * freq_of(lax.rem(n64, own), per * g + n64 // own).astype(f32) + 1.0
            ) * unit
            rec = 1.0 / (e_col * e_col + om * om)
            gr, gi = -e_col * rec, -om * rec
            first = ln < gn
            ga = jnp.where(first, gr, -gi)
            gb = jnp.where(first, gi, gr)
            for i in range(NO):
                cr, ci = pt[0, 0:rows, i : i + 1], pt[1, 0:rows, i : i + 1]
                th, tl = split(ga * cr + gb * ci)
                lh[g, 0:rows, LN * i : LN * i + LN] = th
                ll[g, 0:rows, LN * i : LN * i + LN] = tl
                th, tl = split(gb * cr - ga * ci)
                lh[g, rows : 2 * rows, LN * i : LN * i + LN] = th
                ll[g, rows : 2 * rows, LN * i : LN * i + LN] = tl
            return 0

        lax.fori_loop(0, groups // 2, left, 0)
        far_relay(s_all, s_rows, s_sems)
        lax.fori_loop(groups // 2, groups, left, 0)

        sel = one_hot(
            (iota((NO * JP, LN), 1) == NO * (iota((NO * JP, LN), 0) // JP) + lax.rem(iota((NO * JP, LN), 0), JP))
            & (lax.rem(iota((NO * JP, LN), 0), JP) < NO)
        )

        def arrive(dst, sems, source):
            @pl.when(source != pos)
            def _():
                near_copy(dst, dst, source, source, sems).wait_recv()

        def wait_all(dst, sems):
            def one(source, _):
                arrive(dst, sems, source)
                return 0

            lax.fori_loop(0, near, one, 0)

        def sent_all(src, sems):
            def one(off, _):
                near_copy(src, src, peer(off), pos, sems).wait_send()
                return 0

            lax.fori_loop(1, near, one, 0)

        def cube(x):
            return x.reshape(NO, JP, batch)

        def flat(x):
            return x.reshape(NO * JP, batch)

        wait_all(recv_a, a_sems)
        hyb = [
            cube(dot(sel, recv_a[:, c * own : (c + 1) * own, :].reshape(batch, LN), 1, 1))
            for c in range(2)
        ]
        ainv_r, ainv_i = invert(*hyb)

        far_end(s_all, s_rows, s_sems)
        s_flat = dot(sel, s_all[...].reshape(SEGS * s_rows, LN), 1, 1)
        at_row = iota((SEGS * s_rows, batch), 0)
        slot = lax.rem(iota((SEGS * s_rows, batch), 1), own)

        def spread(kind, c):
            hit = (at_row // s_rows == slot // nf) & (
                lax.rem(at_row, s_rows) == 2 * nf * kind + nf * c + lax.rem(slot, nf)
            )
            return dot(s_flat, one_hot(hit), 1, 0)

        sg_r, sg_i = spread(0, 0), spread(0, 1)
        im_r, im_i = spread(1, 0), spread(1, 1)
        gorb = invert(ainv_r - cube(sg_r), ainv_i - cube(sg_i))
        pick = one_hot(lax.rem(iota((own, batch), 1), own) == iota((own, batch), 0))
        sums = [dot(dot(pick, flat(x), 1, 1), sel, 1, 0) for x in gorb]
        part[seg, 0:own, :] = sums[0]
        part[seg, own : 2 * own, :] = sums[1]
        far_start(part, 2 * own, p_sems)
        far_relay(part, 2 * own, p_sems)
        sent_all(send_a, a_sems)
        far_end(part, 2 * own, p_sems)
        total = (part[0] + part[1] + part[2] + part[3]) * (1.0 / devices)
        t_flat = dot(sel, total, 1, 1)
        t_row = iota((2 * own, batch), 0)
        t_slot = lax.rem(iota((2 * own, batch), 1), own)
        loc = [cube(dot(t_flat, one_hot(t_row == t_slot + own * c), 1, 0)) for c in range(2)]
        linv_r, linv_i = invert(*loc)
        d_r, d_i = flat(linv_r) - im_r, flat(linv_i) - im_i
        q0, q1 = iota((NO * JP, NO * JP), 0), iota((NO * JP, NO * JP), 1)
        same = one_hot(q0 == q1)
        turned = one_hot((q0 // JP == lax.rem(q1, JP)) & (lax.rem(q0, JP) == q1 // JP))
        new_r = sg_r + dot(0.5 * (same + turned), d_r, 1, 0)
        new_i = sg_i + dot(0.5 * (same - turned), d_i, 1, 0)

        own_row = iota((8, batch), 0)
        own_lane = iota((8, batch), 1)
        last = one_hot((own_lane == own - 1) & (own_row == 0))
        last_r = dot(dot(last, new_r, 1, 1), sel, 1, 0)
        last_i = dot(dot(last, new_i, 1, 1), sel, 1, 0)
        h_src[...] = last_r + pltpu.roll(last_i, 1, 0)

        def h_copy(off, sem):
            return pltpu.make_async_remote_copy(
                src_ref=h_src,
                dst_ref=h_dst,
                send_sem=hs_sem.at[sem],
                recv_sem=hr_sem,
                device_id={"ka": base + peer(off)},
                device_id_type=MESH,
            )

        @pl.when(pos == near - 1)
        def _():
            for off in range(1, near):
                h_copy(off, off).start()
            keep = pltpu.make_async_copy(h_src, h_dst, loc_sem)
            keep.start()
            keep.wait()

        gnew = invert(ainv_r - cube(new_r), ainv_i - cube(new_i))
        sn = cube(new_r), cube(new_i)
        half = cmul(*sn, *gnew)
        full = cmul(*half, *sn)
        for c in range(2):
            x = dot(flat(sn[c] + full[c]), sel, 0, 0)
            send_x[:, c * own : (c + 1) * own, :] = x.reshape(near, own, LN)
        near_start(send_x, recv_x, x_sems)
        recv_x[pos] = send_x[pos]

        mine_hit = (own_row < nf) & (own_lane == nf * seg + own_row)
        mine = one_hot(mine_hit)
        for c, value in enumerate((new_r, new_i)):
            lines = dot(dot(mine, value, 1, 1), sel, 1, 0)
            for i in range(NO):
                place = one_hot(iota((NO, LN), 1) == NO * i + iota((NO, LN), 0))
                out_ref[c, i] = dot(lines, place, 1, 1)[0:nf]

        @pl.when(pos != near - 1)
        def _():
            h_copy(1, 0).wait_recv()

        def square(line):
            wide = jnp.broadcast_to(line, (JP, LN))
            return dot(wide * oh_i, oh_j, 1, 1), dot(wide * oh_j, oh_i, 1, 1)

        m_r, mt_r = square(h_dst[0:1, :])
        m_i, mt_i = square(h_dst[1:2, :])
        h_r, h_i = 0.5 * (m_r + mt_r), 0.5 * (m_i - mt_i)
        hp_r = dot(h_r, pr, 1, 0) - dot(h_i, pi, 1, 0)
        hp_i = dot(h_r, pi, 1, 0) + dot(h_i, pr, 1, 0)
        ptr, pti = pt[0], pt[1]
        quad_r = dot(ptr, hp_r, 1, 0) + dot(pti, hp_i, 1, 0)
        quad_i = dot(ptr, hp_i, 1, 0) - dot(pti, hp_r, 1, 0)

        pjt_r, pjt_i = dot(oh_j, pr, 0, 0), dot(oh_j, pi, 0, 0)
        wr = split(jnp.concatenate([pjt_r, -pjt_i], axis=0))
        wi = split(jnp.concatenate([pjt_i, pjt_r], axis=0))
        cacc[...] = jnp.zeros_like(cacc)

        def total_of(g, _):
            for t in range(per):
                arrive(recv_x, x_sems, per * g + t)
            block = recv_x[pl.ds(per * g, per), :, :]
            x = jnp.concatenate(
                [block[:, c * own : (c + 1) * own, :].reshape(gn, LN) for c in range(2)], axis=1
            )
            orb = iota((NO, 1, 2 * LN), 0)
            which = lax.rem(iota((NO, 1, 2 * LN), 2), LN) // NO
            xm = jnp.where(which == orb, x[None], 0.0).reshape(NO * gn, 2 * LN)
            xh, xl = split(xm)
            mr = bdot(xh, wr[0]) + bdot(xh, wr[1]) + bdot(xl, wr[0])
            mi = bdot(xh, wi[0]) + bdot(xh, wi[1]) + bdot(xl, wi[0])
            rn = iota((gn, bp), 0)
            om = (
                2.0 * freq_of(lax.rem(rn, own), per * g + rn // own).astype(f32) + 1.0
            ) * unit
            rec = 1.0 / (energy * energy + om * om)
            gr, gi = -energy * rec, -om * rec
            for i in range(NO):
                a, b = mr[gn * i : gn * i + gn], mi[gn * i : gn * i + gn]
                th, tl = split(a * gr - b * gi)
                rh[2 * gn * i : 2 * gn * i + gn, :] = th
                rl[2 * gn * i : 2 * gn * i + gn, :] = tl
                th, tl = split(a * gi + b * gr)
                rh[2 * gn * i + gn : 2 * gn * i + 2 * gn, :] = th
                rl[2 * gn * i + gn : 2 * gn * i + 2 * gn, :] = tl
            cacc[...] += bdot(lh[g], rh[...]) + bdot(lh[g], rl[...]) + bdot(ll[g], rh[...])
            return 0

        lax.fori_loop(0, groups, total_of, 0)
        c_r = jnp.concatenate([cacc[0:bands, :], jnp.zeros((bp - bands, bp), f32)], axis=0)
        c_i = jnp.concatenate([cacc[rows : rows + bands, :], jnp.zeros((bp - bands, bp), f32)], axis=0)
        scale = 1.0 / inverse_temp
        d0 = (c_r + c_r.T) * scale - weight * quad_r
        d1 = (c_i - c_i.T) * scale - weight * quad_i
        dens_ref[0, 0] = d0[0:bands, 0:bands]
        dens_ref[0, 1] = d1[0:bands, 0:bands]

        sent_all(send_x, x_sems)

        @pl.when(pos == near - 1)
        def _():
            for off in range(1, near):
                h_copy(off, off).wait_send()

    dma = pltpu.SemaphoreType.DMA
    return pl.pallas_call(
        kernel,
        out_shape=(
            jax.ShapeDtypeStruct((1, 2, bands, bands), f32),
            jax.ShapeDtypeStruct((2, NO, nf, NO), f32),
        ),
        in_specs=[pl.BlockSpec(memory_space=pltpu.SMEM)]
        + [pl.BlockSpec(memory_space=pltpu.VMEM)] * 4,
        out_specs=(pl.BlockSpec(memory_space=pltpu.VMEM),) * 2,
        scratch_shapes=[
            pltpu.VMEM((2, JP, bp), f32),
            pltpu.VMEM((2, bp, JP), f32),
            pltpu.VMEM((8, bp), f32),
            pltpu.VMEM((NO, 4 * nf, NO), f32),
            pltpu.VMEM((SEGS, 4 * nf, LN), f32),
            pltpu.VMEM((SEGS, 2 * own, LN), f32),
            pltpu.VMEM((near, 2 * own, LN), f32),
            pltpu.VMEM((near, 2 * own, LN), f32),
            pltpu.VMEM((near, 2 * own, LN), f32),
            pltpu.VMEM((near, 2 * own, LN), f32),
            pltpu.VMEM((8, LN), f32),
            pltpu.VMEM((8, LN), f32),
            pltpu.VMEM((groups, 2 * rows, NO * LN), bf16),
            pltpu.VMEM((groups, 2 * rows, NO * LN), bf16),
            pltpu.VMEM((NO * LN, bp), bf16),
            pltpu.VMEM((NO * LN, bp), bf16),
            pltpu.VMEM((2 * rows, bp), f32),
            dma((near,)), dma((near,)), dma((near,)), dma((near,)),
            dma((4,)), dma((4,)), dma((4,)), dma((4,)),
            dma((near,)), dma, dma,
        ],
        compiler_params=pltpu.CompilerParams(
            collective_id=0, has_side_effects=True, vmem_limit_bytes=48 * 1024 * 1024
        ),
        name="charge_update",
    )


def solution(mesh):
    devices = mesh.shape["ka"]

    def local(energies, proj, window, sigma, impurity_inverse):
        call = build(devices, sigma.shape[3], energies.shape[1])
        density, new = call(
            window,
            energies,
            jnp.swapaxes(proj, 1, 2),
            jnp.swapaxes(sigma, 2, 3),
            jnp.swapaxes(impurity_inverse, 2, 3),
        )
        return density, jnp.swapaxes(new, 2, 3)

    both = ("parts", "ka")
    in_specs = (
        P(both, None),
        P(both, None, None, None),
        P(both, None),
        P("parts", None, None, "ka"),
        P("parts", None, None, "ka"),
    )
    out_specs = (P(both, None, None, None), P("parts", None, None, "ka"))
    return jax.shard_map(local, mesh=mesh, in_specs=in_specs, out_specs=out_specs, check_vma=False)
```

```python
import math

import jax
import jax.numpy as jnp
from jax import lax
from jax.experimental import pallas as pl
from jax.experimental.pallas import tpu as pltpu
from jax.sharding import PartitionSpec as P

f32 = jnp.float32
bf16 = jnp.bfloat16
HI = lax.Precision.HIGHEST
MESH = pl.DeviceIdType.MESH
inverse_temp = 40.0
SEGS = 4
NO = 10
JP = 16
LN = 128


def tail_weight(count):
    total = 0.0
    for number in range(count):
        total += (inverse_temp / (math.pi * (2 * number + 1))) ** 2
    return inverse_temp / 4.0 - 2.0 / inverse_temp * total


def dot(a, b, ca, cb):
    return lax.dot_general(
        a, b, (((ca,), (cb,)), ((), ())), precision=HI, preferred_element_type=f32
    )


def bdot(a, b):
    return jnp.dot(a, b, preferred_element_type=f32)


def split(x):
    high = x.astype(bf16)
    return high, (x - high.astype(f32)).astype(bf16)


def iota(shape, dim):
    return lax.broadcasted_iota(jnp.int32, shape, dim)


def one_hot(cond):
    return jnp.where(cond, 1.0, 0.0).astype(f32)


def placed(array, line, p):
    pieces = [array[:p]] if p else []
    pieces.append(line)
    if p + 1 < array.shape[0]:
        pieces.append(array[p + 1 :])
    return jnp.concatenate(pieces, axis=0)


def invert(ar, ai):
    cols = iota(ar.shape, 1)
    for p in range(NO):
        pr, pi = ar[p : p + 1, p : p + 1, :], ai[p : p + 1, p : p + 1, :]
        inv = 1.0 / (pr * pr + pi * pi)
        rr, ri = pr * inv, -pi * inv
        rowr, rowi = ar[p : p + 1], ai[p : p + 1]
        at = cols[p : p + 1] == p
        nr = jnp.where(at, rr, rowr * rr - rowi * ri)
        ni = jnp.where(at, ri, rowr * ri + rowi * rr)
        cr, ci = ar[:, p : p + 1, :], ai[:, p : p + 1, :]
        br = jnp.where(cols == p, 0.0, ar)
        bi = jnp.where(cols == p, 0.0, ai)
        br = br - (cr * nr - ci * ni)
        bi = bi - (cr * ni + ci * nr)
        ar, ai = placed(br, nr, p), placed(bi, ni, p)
    return ar, ai


def cmul(ar, ai, br, bi):
    outr = outi = None
    for l in range(NO):
        xr, xi = ar[:, l : l + 1, :], ai[:, l : l + 1, :]
        yr, yi = br[l : l + 1], bi[l : l + 1]
        tr, ti = xr * yr - xi * yi, xr * yi + xi * yr
        outr = tr if outr is None else outr + tr
        outi = ti if outi is None else outi + ti
    return outr, outi


def build(devices, nf, bands):
    near = devices // SEGS
    own = SEGS * nf
    batch = near * own
    bp = (bands + LN - 1) // LN * LN
    rows = (bands + 15) // 16 * 16
    count = devices * nf
    step = near * nf
    per = 4
    groups = near // per
    gn = per * own
    weight = tail_weight(count)
    dense = 2 * own * NO * NO // LN
    cut = 2 * own
    unit = math.pi / inverse_temp

    def freq_of(slot, place):
        return step * (slot // nf) + nf * place + slot % nf

    def kernel(
        w_hbm, e_hbm, proj_hbm, sig_hbm, imp_hbm, dens_ref, out_ref,
        w_ref, e_ref, proj_ref, sig_ref, imp_ref,
        p16, pt, e2, sfix, gsr, gsi, masks, s_all, part, send_a, recv_a, send_x, recv_x, h_src, h_dst,
        lh, ll, rh, rl, cacc,
        as_sem, ar_sem, xs_sem, xr_sem, ss_sem, sr_sem, ps_sem, pr_sem, hs_sem, hr_sem, loc_sem, in_sem,
    ):
        me = lax.axis_index("ka")
        seg = me // near
        pos = lax.rem(me, near)
        base = seg * near
        up = lax.rem(me + near, devices)
        down = lax.rem(me + devices - near, devices)
        seg_up = lax.rem(seg + 1, SEGS)
        seg_down = lax.rem(seg + SEGS - 1, SEGS)
        seg_far = lax.rem(seg + 2, SEGS)

        def peer(off):
            return lax.rem(pos + off, near)

        sources = (e_hbm, proj_hbm, w_hbm, sig_hbm, imp_hbm)
        targets = (e_ref, proj_ref, w_ref, sig_ref, imp_ref)
        loads = [
            pltpu.make_async_copy(a, b, in_sem.at[k])
            for k, (a, b) in enumerate(zip(sources, targets))
        ]
        for load in loads:
            load.start()
        recv_a[:, dense - 1 : 2 * own, :] = jnp.zeros((near, 2 * own - dense + 1, LN), f32)

        barrier = pltpu.get_barrier_semaphore()
        for target in (up, down):
            pl.semaphore_signal(barrier, inc=1, device_id={"ka": target}, device_id_type=MESH)

        def greet(off, _):
            pl.semaphore_signal(
                barrier, inc=1, device_id={"ka": base + peer(off)}, device_id_type=MESH
            )
            return 0

        lax.fori_loop(1, near, greet, 0)

        p16[...] = jnp.zeros_like(p16)
        e2[...] = jnp.zeros_like(e2)
        sfix[...] = jnp.zeros_like(sfix)
        for load in loads:
            load.wait()
        lane = iota((1, bands), 1)
        inside = one_hot((lane >= w_ref[0:1, 0:1]) & (lane < w_ref[0:1, 1:2]))
        e2[0:1, 0:bands] = e_ref[...]
        for c in range(2):
            for i in range(NO):
                p16[c, i : i + 1, 0:bands] = proj_ref[0, i, c : c + 1, :] * inside
        for kind, ref in enumerate((sig_ref, imp_ref)):
            for c in range(2):
                for i in range(NO):
                    at = 2 * nf * kind + nf * c
                    sfix[i, at : at + nf, 0:NO] = ref[c, i]
        packed = None
        for i in range(NO):
            term = pltpu.roll(sfix[i], NO * i, 1) if i else sfix[i]
            packed = term if packed is None else packed + term
        s_all[seg] = packed

        oh_i = one_hot((iota((JP, LN), 1) // NO == iota((JP, LN), 0)) & (iota((JP, LN), 1) < NO * NO))
        oh_j = one_hot(
            (lax.rem(iota((JP, LN), 1), NO) == iota((JP, LN), 0)) & (iota((JP, LN), 1) < NO * NO)
        )
        pr, pi = p16[0], p16[1]
        eye = one_hot(iota((JP, JP), 0) == iota((JP, JP), 1))
        pt[0] = dot(pr, eye, 0, 0)
        pt[1] = dot(pi, eye, 0, 0)

        dr = iota((LN, JP), 0)
        di = dense * (dr // cut) + lax.rem(dr, cut)
        real = lax.rem(dr, cut) < dense
        ex_i = one_hot((di // NO == iota((LN, JP), 1)) & real)
        ex_j = one_hot((lax.rem(di, NO) == iota((LN, JP), 1)) & real)
        pir, pii = dot(ex_i, pr, 1, 0), dot(ex_i, pi, 1, 0)
        pjr, pji = dot(ex_j, pr, 1, 0), dot(ex_j, pi, 1, 0)
        ppr = pir * pjr + pii * pji
        ppi = pii * pjr - pir * pji
        row = iota((near * cut, bp), 0)
        num = freq_of(lax.rem(row, own), row // cut)
        omega = (2.0 * num.astype(f32) + 1.0) * unit
        energy = e2[0:1, :]
        recip = 1.0 / (energy * energy + omega * omega)
        g1, g2 = -energy * recip, -omega * recip
        real_row = lax.rem(row // own, 2) == 0
        a_all = dot(ppr, jnp.where(real_row, g1, g2), 1, 1) + dot(
            ppi, jnp.where(real_row, -g2, g1), 1, 1
        )
        quarter = iota((cut, LN), 1) // cut
        for far_place in range(near // 4):
            for place in range(4):
                block = None
                for q in range(4):
                    piece = a_all[cut * q : cut * q + cut, LN * far_place : LN * far_place + LN]
                    turn = (cut * (q - place)) % LN
                    piece = pltpu.roll(piece, turn, 1) if turn else piece
                    block = piece if block is None else jnp.where(quarter == q, piece, block)
                send_a[4 * far_place + place] = block

        pl.semaphore_wait(barrier, near + 1)

        def far_copy(buf, index, lo, size, sems, sem, target):
            return pltpu.make_async_remote_copy(
                src_ref=buf.at[index, pl.ds(lo, size), :],
                dst_ref=buf.at[index, pl.ds(lo, size), :],
                send_sem=sems[0].at[sem],
                recv_sem=sems[1].at[sem],
                device_id={"ka": target},
                device_id_type=MESH,
            )

        def far_start(buf, size, sems):
            far_copy(buf, seg, 0, size, sems, 0, up).start()
            far_copy(buf, seg, 0, size, sems, 1, down).start()

        def far_relay(buf, size, sems):
            half = size // 2
            far_copy(buf, seg_down, 0, size, sems, 0, up).wait_recv()
            far_copy(buf, seg_down, 0, half, sems, 2, up).start()
            far_copy(buf, seg_up, 0, size, sems, 1, down).wait_recv()
            far_copy(buf, seg_up, half, half, sems, 3, down).start()

        def far_end(buf, size, sems):
            half = size // 2
            far_copy(buf, seg_far, 0, half, sems, 2, up).wait_recv()
            far_copy(buf, seg_far, half, half, sems, 3, down).wait_recv()
            far_copy(buf, seg, 0, size, sems, 0, up).wait_send()
            far_copy(buf, seg, 0, size, sems, 1, down).wait_send()
            far_copy(buf, seg_down, 0, half, sems, 2, up).wait_send()
            far_copy(buf, seg_up, half, half, sems, 3, down).wait_send()

        def near_copy(src, dst, to, source, sems, size):
            return pltpu.make_async_remote_copy(
                src_ref=src.at[to, pl.ds(0, size), :],
                dst_ref=dst.at[source, pl.ds(0, size), :],
                send_sem=sems[0].at[to],
                recv_sem=sems[1].at[source],
                device_id={"ka": base + to},
                device_id_type=MESH,
            )

        def at_turn(turn):
            return lax.rem(
                pos + near + near // 2 + (turn + 1) // 2 * (1 - 2 * lax.rem(turn, 2)), near
            )

        def near_start(src, dst, sems, size):
            for turn in range(near - 1):
                off = near // 2 + (turn + 1) // 2 * (1 - 2 * (turn % 2))
                near_copy(src, dst, peer(off), pos, sems, size).start()

        s_sems, p_sems = (ss_sem, sr_sem), (ps_sem, pr_sem)
        a_sems, x_sems = (as_sem, ar_sem), (xs_sem, xr_sem)
        s_rows = 4 * nf
        far_start(s_all, s_rows, s_sems)
        near_start(send_a, recv_a, a_sems, dense)
        recv_a[pos] = send_a[pos]
        orb = iota((NO, gn, 2 * LN), 0)
        which = lax.rem(iota((NO, gn, 2 * LN), 2), LN) // NO
        masks[...] = one_hot(which == orb).astype(bf16)

        e_col = dot(e2[0:1, :], jnp.ones((1, LN), f32), 0, 0)[0:rows]

        def omega_of(number, g):
            place = at_turn(per * g + number // own)
            return (2.0 * freq_of(lax.rem(number, own), place).astype(f32) + 1.0) * unit

        def left(g, _):
            om = omega_of(iota((gn, bp), 0), g)
            rec = 1.0 / (energy * energy + om * om)
            gsr[g] = -energy * rec
            gsi[g] = -om * rec
            ln = iota((rows, LN), 1)
            n64 = lax.rem(ln, gn)
            om = omega_of(n64, g)
            rec = 1.0 / (e_col * e_col + om * om)
            gr, gi = -e_col * rec, -om * rec
            first = ln < gn
            ga = jnp.where(first, gr, -gi)
            gb = jnp.where(first, gi, gr)
            for i in range(NO):
                cr, ci = pt[0, 0:rows, i : i + 1], pt[1, 0:rows, i : i + 1]
                th, tl = split(ga * cr + gb * ci)
                lh[g, 0:rows, LN * i : LN * i + LN] = th
                ll[g, 0:rows, LN * i : LN * i + LN] = tl
                th, tl = split(gb * cr - ga * ci)
                lh[g, rows : 2 * rows, LN * i : LN * i + LN] = th
                ll[g, rows : 2 * rows, LN * i : LN * i + LN] = tl
            return 0

        lax.fori_loop(0, groups // 2, left, 0)
        far_relay(s_all, s_rows, s_sems)
        lax.fori_loop(groups // 2, groups, left, 0)

        sel = one_hot(
            (iota((NO * JP, LN), 1) == NO * (iota((NO * JP, LN), 0) // JP) + lax.rem(iota((NO * JP, LN), 0), JP))
            & (lax.rem(iota((NO * JP, LN), 0), JP) < NO)
        )

        def arrive(dst, sems, source, size):
            @pl.when(source != pos)
            def _():
                near_copy(dst, dst, source, source, sems, size).wait_recv()

        def wait_all(dst, sems, size):
            def one(source, _):
                arrive(dst, sems, source, size)
                return 0

            lax.fori_loop(0, near, one, 0)

        def sent_all(src, sems, size):
            def one(off, _):
                near_copy(src, src, peer(off), pos, sems, size).wait_send()
                return 0

            lax.fori_loop(1, near, one, 0)

        def cube(x):
            return x.reshape(NO, JP, batch)

        def flat(x):
            return x.reshape(NO * JP, batch)

        sr = iota((NO * JP, LN), 0)
        sc = iota((NO * JP, LN), 1)
        to_cube = one_hot(
            (dense * (sc // cut) + lax.rem(sc, cut) == NO * (sr // JP) + lax.rem(sr, JP))
            & (lax.rem(sr, JP) < NO)
            & (lax.rem(sc, cut) < dense)
        )
        eighth = iota((cut, LN), 1) // own

        def gathered(c):
            lines = []
            for q in range(4):
                halves = []
                for far_k in range(near // 8):
                    block = None
                    for k in range(8):
                        piece = recv_a[8 * far_k + k]
                        turn = (own * k - cut * q - own * c) % LN
                        piece = pltpu.roll(piece, turn, 1) if turn else piece
                        block = piece if block is None else jnp.where(eighth == k, piece, block)
                    halves.append(block)
                lines.append(jnp.concatenate(halves, axis=1))
            return cube(dot(to_cube, jnp.concatenate(lines, axis=0), 1, 0))

        wait_all(recv_a, a_sems, dense)
        ainv_r, ainv_i = invert(gathered(0), gathered(1))

        far_end(s_all, s_rows, s_sems)
        s_flat = dot(sel, s_all[...].reshape(SEGS * s_rows, LN), 1, 1)
        at_row = iota((SEGS * s_rows, batch), 0)
        slot = lax.rem(iota((SEGS * s_rows, batch), 1), own)

        def spread(kind, c):
            hit = (at_row // s_rows == slot // nf) & (
                lax.rem(at_row, s_rows) == 2 * nf * kind + nf * c + lax.rem(slot, nf)
            )
            return dot(s_flat, one_hot(hit), 1, 0)

        sg_r, sg_i = spread(0, 0), spread(0, 1)
        im_r, im_i = spread(1, 0), spread(1, 1)
        gorb = invert(ainv_r - cube(sg_r), ainv_i - cube(sg_i))
        pick = one_hot(lax.rem(iota((own, batch), 1), own) == iota((own, batch), 0))
        sums = [dot(dot(pick, flat(x), 1, 1), sel, 1, 0) for x in gorb]
        part[seg, 0:own, :] = sums[0]
        part[seg, own : 2 * own, :] = sums[1]
        far = lax.rem(me + 2 * near, devices)
        far_copy(part, seg, 0, cut, p_sems, 2, far).start()
        far_start(part, cut, p_sems)
        sent_all(send_a, a_sems, dense)
        far_copy(part, seg_down, 0, cut, p_sems, 0, up).wait_recv()
        far_copy(part, seg_up, 0, cut, p_sems, 1, down).wait_recv()
        far_copy(part, seg_far, 0, cut, p_sems, 2, far).wait_recv()
        far_copy(part, seg, 0, cut, p_sems, 0, up).wait_send()
        far_copy(part, seg, 0, cut, p_sems, 1, down).wait_send()
        far_copy(part, seg, 0, cut, p_sems, 2, far).wait_send()
        total = (part[0] + part[1] + part[2] + part[3]) * (1.0 / devices)
        t_flat = dot(sel, total, 1, 1)
        t_row = iota((2 * own, batch), 0)
        t_slot = lax.rem(iota((2 * own, batch), 1), own)
        loc = [cube(dot(t_flat, one_hot(t_row == t_slot + own * c), 1, 0)) for c in range(2)]
        linv_r, linv_i = invert(*loc)
        d_r, d_i = flat(linv_r) - im_r, flat(linv_i) - im_i
        q0, q1 = iota((NO * JP, NO * JP), 0), iota((NO * JP, NO * JP), 1)
        same = one_hot(q0 == q1)
        turned = one_hot((q0 // JP == lax.rem(q1, JP)) & (lax.rem(q0, JP) == q1 // JP))
        new_r = sg_r + dot(0.5 * (same + turned), d_r, 1, 0)
        new_i = sg_i + dot(0.5 * (same - turned), d_i, 1, 0)

        own_row = iota((8, batch), 0)
        own_lane = iota((8, batch), 1)
        last = one_hot((own_lane == own - 1) & (own_row == 0))
        last_r = dot(dot(last, new_r, 1, 1), sel, 1, 0)
        last_i = dot(dot(last, new_i, 1, 1), sel, 1, 0)
        h_src[...] = last_r + pltpu.roll(last_i, 1, 0)

        def h_copy(off, sem):
            return pltpu.make_async_remote_copy(
                src_ref=h_src,
                dst_ref=h_dst,
                send_sem=hs_sem.at[sem],
                recv_sem=hr_sem,
                device_id={"ka": base + peer(off)},
                device_id_type=MESH,
            )

        gnew = invert(ainv_r - cube(new_r), ainv_i - cube(new_i))
        sn = cube(new_r), cube(new_i)
        half = cmul(*sn, *gnew)
        full = cmul(*half, *sn)
        for c in range(2):
            x = dot(flat(sn[c] + full[c]), sel, 0, 0)
            send_x[:, c * own : (c + 1) * own, :] = x.reshape(near, own, LN)
        near_start(send_x, recv_x, x_sems, cut)
        recv_x[pos] = send_x[pos]

        @pl.when(pos == near - 1)
        def _():
            for off in range(1, near):
                h_copy(off, off).start()
            keep = pltpu.make_async_copy(h_src, h_dst, loc_sem)
            keep.start()
            keep.wait()

        mine_hit = (own_row < nf) & (own_lane == nf * seg + own_row)
        mine = one_hot(mine_hit)
        for c, value in enumerate((new_r, new_i)):
            lines = dot(dot(mine, value, 1, 1), sel, 1, 0)
            for i in range(NO):
                place = one_hot(iota((NO, LN), 1) == NO * i + iota((NO, LN), 0))
                out_ref[c, i] = dot(lines, place, 1, 1)[0:nf]

        pjt_r, pjt_i = dot(oh_j, pr, 0, 0), dot(oh_j, pi, 0, 0)
        wr = split(jnp.concatenate([pjt_r, -pjt_i], axis=0))
        wi = split(jnp.concatenate([pjt_i, pjt_r], axis=0))
        cacc[...] = jnp.zeros_like(cacc)

        def total_of(g, _):
            places = [at_turn(per * g + t) for t in range(per)]
            for place in places:
                arrive(recv_x, x_sems, place, cut)
            blocks = [recv_x[place] for place in places]
            x = jnp.concatenate(
                [
                    jnp.concatenate([b[c * own : (c + 1) * own] for b in blocks], axis=0)
                    for c in range(2)
                ],
                axis=1,
            )
            xh, xl = split(x)
            xh = (xh[None] * masks[...]).reshape(NO * gn, 2 * LN)
            xl = (xl[None] * masks[...]).reshape(NO * gn, 2 * LN)
            mr = bdot(xh, wr[0]) + bdot(xh, wr[1]) + bdot(xl, wr[0])
            mi = bdot(xh, wi[0]) + bdot(xh, wi[1]) + bdot(xl, wi[0])
            gr, gi = gsr[g], gsi[g]
            for i in range(NO):
                a, b = mr[gn * i : gn * i + gn], mi[gn * i : gn * i + gn]
                th, tl = split(a * gr - b * gi)
                rh[2 * gn * i : 2 * gn * i + gn, :] = th
                rl[2 * gn * i : 2 * gn * i + gn, :] = tl
                th, tl = split(a * gi + b * gr)
                rh[2 * gn * i + gn : 2 * gn * i + 2 * gn, :] = th
                rl[2 * gn * i + gn : 2 * gn * i + 2 * gn, :] = tl
            cacc[...] += bdot(lh[g], rh[...]) + bdot(lh[g], rl[...]) + bdot(ll[g], rh[...])
            return 0

        lax.fori_loop(0, groups - 1, total_of, 0)

        @pl.when(pos != near - 1)
        def _():
            h_copy(1, 0).wait_recv()

        def square(line):
            wide = jnp.broadcast_to(line, (JP, LN))
            return dot(wide * oh_i, oh_j, 1, 1), dot(wide * oh_j, oh_i, 1, 1)

        m_r, mt_r = square(h_dst[0:1, :])
        m_i, mt_i = square(h_dst[1:2, :])
        h_r, h_i = 0.5 * (m_r + mt_r), 0.5 * (m_i - mt_i)
        hp_r = dot(h_r, pr, 1, 0) - dot(h_i, pi, 1, 0)
        hp_i = dot(h_r, pi, 1, 0) + dot(h_i, pr, 1, 0)
        ptr, pti = pt[0], pt[1]
        quad_r = dot(ptr, hp_r, 1, 0) + dot(pti, hp_i, 1, 0)
        quad_i = dot(ptr, hp_i, 1, 0) - dot(pti, hp_r, 1, 0)

        lax.fori_loop(groups - 1, groups, total_of, 0)
        c_r = jnp.concatenate([cacc[0:bands, :], jnp.zeros((bp - bands, bp), f32)], axis=0)
        c_i = jnp.concatenate([cacc[rows : rows + bands, :], jnp.zeros((bp - bands, bp), f32)], axis=0)
        scale = 1.0 / inverse_temp
        d0 = (c_r + c_r.T) * scale - weight * quad_r
        d1 = (c_i - c_i.T) * scale - weight * quad_i
        dens_ref[0, 0] = d0[0:bands, 0:bands]
        dens_ref[0, 1] = d1[0:bands, 0:bands]

        sent_all(send_x, x_sems, cut)

        @pl.when(pos == near - 1)
        def _():
            for off in range(1, near):
                h_copy(off, off).wait_send()

    dma = pltpu.SemaphoreType.DMA
    return pl.pallas_call(
        kernel,
        out_shape=(
            jax.ShapeDtypeStruct((1, 2, bands, bands), f32),
            jax.ShapeDtypeStruct((2, NO, nf, NO), f32),
        ),
        in_specs=[pl.BlockSpec(memory_space=pltpu.HBM)] * 5,
        out_specs=(pl.BlockSpec(memory_space=pltpu.VMEM),) * 2,
        scratch_shapes=[
            pltpu.VMEM((1, 2), jnp.int32),
            pltpu.VMEM((1, bands), f32),
            pltpu.VMEM((1, NO, 2, bands), f32),
            pltpu.VMEM((2, NO, nf, NO), f32),
            pltpu.VMEM((2, NO, nf, NO), f32),
            pltpu.VMEM((2, JP, bp), f32),
            pltpu.VMEM((2, bp, JP), f32),
            pltpu.VMEM((8, bp), f32),
            pltpu.VMEM((NO, 4 * nf, LN), f32),
            pltpu.VMEM((groups, gn, bp), f32),
            pltpu.VMEM((groups, gn, bp), f32),
            pltpu.VMEM((NO, gn, 2 * LN), bf16),
            pltpu.VMEM((SEGS, 4 * nf, LN), f32),
            pltpu.VMEM((SEGS, 2 * own, LN), f32),
            pltpu.VMEM((near, 2 * own, LN), f32),
            pltpu.VMEM((near, 2 * own, LN), f32),
            pltpu.VMEM((near, 2 * own, LN), f32),
            pltpu.VMEM((near, 2 * own, LN), f32),
            pltpu.VMEM((8, LN), f32),
            pltpu.VMEM((8, LN), f32),
            pltpu.VMEM((groups, 2 * rows, NO * LN), bf16),
            pltpu.VMEM((groups, 2 * rows, NO * LN), bf16),
            pltpu.VMEM((NO * LN, bp), bf16),
            pltpu.VMEM((NO * LN, bp), bf16),
            pltpu.VMEM((2 * rows, bp), f32),
            dma((near,)), dma((near,)), dma((near,)), dma((near,)),
            dma((4,)), dma((4,)), dma((4,)), dma((4,)),
            dma((near,)), dma, dma, dma((5,)),
        ],
        compiler_params=pltpu.CompilerParams(
            collective_id=0, has_side_effects=True, vmem_limit_bytes=67043328
        ),
        name="charge_update",
    )


def solution(mesh):
    devices = mesh.shape["ka"]

    def local(energies, proj, window, sigma, impurity_inverse):
        call = build(devices, sigma.shape[3], energies.shape[1])
        density, new = call(
            window,
            energies,
            jnp.swapaxes(proj, 1, 2),
            jnp.swapaxes(sigma, 2, 3),
            jnp.swapaxes(impurity_inverse, 2, 3),
        )
        return density, jnp.swapaxes(new, 2, 3)

    both = ("parts", "ka")
    in_specs = (
        P(both, None),
        P(both, None, None, None),
        P(both, None),
        P("parts", None, None, "ka"),
        P("parts", None, None, "ka"),
    )
    out_specs = (P(both, None, None, None), P("parts", None, None, "ka"))
    return jax.shard_map(local, mesh=mesh, in_specs=in_specs, out_specs=out_specs, check_vma=False)
```

```python
import math

import jax
import jax.numpy as jnp
from jax import lax
from jax.experimental import pallas as pl
from jax.experimental.pallas import tpu as pltpu
from jax.sharding import PartitionSpec as P

f32 = jnp.float32
bf16 = jnp.bfloat16
HI = lax.Precision.HIGHEST
MESH = pl.DeviceIdType.MESH
inverse_temp = 40.0
SEGS = 4
NO = 10
JP = 16
LN = 128


def tail_weight(count):
    total = 0.0
    for number in range(count):
        total += (inverse_temp / (math.pi * (2 * number + 1))) ** 2
    return inverse_temp / 4.0 - 2.0 / inverse_temp * total


def dot(a, b, ca, cb):
    return lax.dot_general(
        a, b, (((ca,), (cb,)), ((), ())), precision=HI, preferred_element_type=f32
    )


def bdot(a, b):
    return jnp.dot(a, b, preferred_element_type=f32)


def split(x):
    high = x.astype(bf16)
    return high, (x - high.astype(f32)).astype(bf16)


def iota(shape, dim):
    return lax.broadcasted_iota(jnp.int32, shape, dim)


def one_hot(cond):
    return jnp.where(cond, 1.0, 0.0).astype(f32)


def placed(array, line, p):
    pieces = [array[:p]] if p else []
    pieces.append(line)
    if p + 1 < array.shape[0]:
        pieces.append(array[p + 1 :])
    return jnp.concatenate(pieces, axis=0)


def invert(ar, ai):
    cols = iota(ar.shape, 1)
    for p in range(NO):
        pr, pi = ar[p : p + 1, p : p + 1, :], ai[p : p + 1, p : p + 1, :]
        inv = 1.0 / (pr * pr + pi * pi)
        rr, ri = pr * inv, -pi * inv
        rowr, rowi = ar[p : p + 1], ai[p : p + 1]
        at = cols[p : p + 1] == p
        nr = jnp.where(at, rr, rowr * rr - rowi * ri)
        ni = jnp.where(at, ri, rowr * ri + rowi * rr)
        cr, ci = ar[:, p : p + 1, :], ai[:, p : p + 1, :]
        br = jnp.where(cols == p, 0.0, ar)
        bi = jnp.where(cols == p, 0.0, ai)
        br = br - (cr * nr - ci * ni)
        bi = bi - (cr * ni + ci * nr)
        ar, ai = placed(br, nr, p), placed(bi, ni, p)
    return ar, ai


def cmul(ar, ai, br, bi):
    outr = outi = None
    for l in range(NO):
        xr, xi = ar[:, l : l + 1, :], ai[:, l : l + 1, :]
        yr, yi = br[l : l + 1], bi[l : l + 1]
        tr, ti = xr * yr - xi * yi, xr * yi + xi * yr
        outr = tr if outr is None else outr + tr
        outi = ti if outi is None else outi + ti
    return outr, outi


def build(devices, nf, bands):
    near = devices // SEGS
    own = SEGS * nf
    batch = near * own
    bp = (bands + LN - 1) // LN * LN
    rows = (bands + 15) // 16 * 16
    count = devices * nf
    step = near * nf
    per = 4
    groups = near // per
    gn = per * own
    weight = tail_weight(count)
    dense = 2 * own * NO * NO // LN
    cut = 2 * own
    unit = math.pi / inverse_temp

    def freq_of(slot, place):
        return step * (slot // nf) + nf * place + slot % nf

    def kernel(
        w_hbm, e_hbm, proj_hbm, sig_hbm, imp_hbm, dens_ref, out_ref,
        w_ref, e_ref, proj_ref, sig_ref, imp_ref,
        p16, pt, e2, sfix, gsr, gsi, masks, s_all, part, send_a, recv_a, send_x, recv_x, h_src, h_dst,
        lcat, rcat, wcat, cacc,
        as_sem, ar_sem, xs_sem, xr_sem, ss_sem, sr_sem, ps_sem, pr_sem, hs_sem, hr_sem, loc_sem, in_sem,
    ):
        me = lax.axis_index("ka")
        seg = me // near
        pos = lax.rem(me, near)
        base = seg * near
        up = lax.rem(me + near, devices)
        down = lax.rem(me + devices - near, devices)
        seg_up = lax.rem(seg + 1, SEGS)
        seg_down = lax.rem(seg + SEGS - 1, SEGS)
        seg_far = lax.rem(seg + 2, SEGS)

        def peer(off):
            return lax.rem(pos + off, near)

        sources = (e_hbm, proj_hbm, w_hbm, sig_hbm, imp_hbm)
        targets = (e_ref, proj_ref, w_ref, sig_ref, imp_ref)
        loads = [
            pltpu.make_async_copy(a, b, in_sem.at[k])
            for k, (a, b) in enumerate(zip(sources, targets))
        ]
        for load in loads:
            load.start()
        recv_a[:, dense - 1 : 2 * own, :] = jnp.zeros((near, 2 * own - dense + 1, LN), f32)

        barrier = pltpu.get_barrier_semaphore()
        for target in (up, down):
            pl.semaphore_signal(barrier, inc=1, device_id={"ka": target}, device_id_type=MESH)

        def greet(off, _):
            pl.semaphore_signal(
                barrier, inc=1, device_id={"ka": base + peer(off)}, device_id_type=MESH
            )
            return 0

        lax.fori_loop(1, near, greet, 0)

        p16[...] = jnp.zeros_like(p16)
        e2[...] = jnp.zeros_like(e2)
        sfix[...] = jnp.zeros_like(sfix)
        for load in loads:
            load.wait()
        lane = iota((1, bands), 1)
        inside = one_hot((lane >= w_ref[0:1, 0:1]) & (lane < w_ref[0:1, 1:2]))
        e2[0:1, 0:bands] = e_ref[...]
        for c in range(2):
            for i in range(NO):
                p16[c, i : i + 1, 0:bands] = proj_ref[0, i, c : c + 1, :] * inside
        for kind, ref in enumerate((sig_ref, imp_ref)):
            for c in range(2):
                for i in range(NO):
                    at = 2 * nf * kind + nf * c
                    sfix[i, at : at + nf, 0:NO] = ref[c, i]
        packed = None
        for i in range(NO):
            term = pltpu.roll(sfix[i], NO * i, 1) if i else sfix[i]
            packed = term if packed is None else packed + term
        s_all[seg] = packed

        oh_i = one_hot((iota((JP, LN), 1) // NO == iota((JP, LN), 0)) & (iota((JP, LN), 1) < NO * NO))
        oh_j = one_hot(
            (lax.rem(iota((JP, LN), 1), NO) == iota((JP, LN), 0)) & (iota((JP, LN), 1) < NO * NO)
        )
        pr, pi = p16[0], p16[1]
        eye = one_hot(iota((JP, JP), 0) == iota((JP, JP), 1))
        pt[0] = dot(pr, eye, 0, 0)
        pt[1] = dot(pi, eye, 0, 0)

        dr = iota((LN, JP), 0)
        di = dense * (dr // cut) + lax.rem(dr, cut)
        real = lax.rem(dr, cut) < dense
        ex_i = one_hot((di // NO == iota((LN, JP), 1)) & real)
        ex_j = one_hot((lax.rem(di, NO) == iota((LN, JP), 1)) & real)
        pir, pii = dot(ex_i, pr, 1, 0), dot(ex_i, pi, 1, 0)
        pjr, pji = dot(ex_j, pr, 1, 0), dot(ex_j, pi, 1, 0)
        ppr = pir * pjr + pii * pji
        ppi = pii * pjr - pir * pji
        row = iota((near * cut, bp), 0)
        num = freq_of(lax.rem(row, own), row // cut)
        omega = (2.0 * num.astype(f32) + 1.0) * unit
        energy = e2[0:1, :]
        recip = 1.0 / (energy * energy + omega * omega)
        g1, g2 = -energy * recip, -omega * recip
        real_row = lax.rem(row // own, 2) == 0
        a_all = dot(ppr, jnp.where(real_row, g1, g2), 1, 1) + dot(
            ppi, jnp.where(real_row, -g2, g1), 1, 1
        )
        quarter = iota((cut, LN), 1) // cut
        for far_place in range(near // 4):
            for place in range(4):
                block = None
                for q in range(4):
                    piece = a_all[cut * q : cut * q + cut, LN * far_place : LN * far_place + LN]
                    turn = (cut * (q - place)) % LN
                    piece = pltpu.roll(piece, turn, 1) if turn else piece
                    block = piece if block is None else jnp.where(quarter == q, piece, block)
                send_a[4 * far_place + place] = block

        pl.semaphore_wait(barrier, near + 1)

        def far_copy(buf, index, lo, size, sems, sem, target):
            return pltpu.make_async_remote_copy(
                src_ref=buf.at[index, pl.ds(lo, size), :],
                dst_ref=buf.at[index, pl.ds(lo, size), :],
                send_sem=sems[0].at[sem],
                recv_sem=sems[1].at[sem],
                device_id={"ka": target},
                device_id_type=MESH,
            )

        def far_start(buf, size, sems):
            far_copy(buf, seg, 0, size, sems, 0, up).start()
            far_copy(buf, seg, 0, size, sems, 1, down).start()

        def far_relay(buf, size, sems):
            half = size // 2
            far_copy(buf, seg_down, 0, size, sems, 0, up).wait_recv()
            far_copy(buf, seg_down, 0, half, sems, 2, up).start()
            far_copy(buf, seg_up, 0, size, sems, 1, down).wait_recv()
            far_copy(buf, seg_up, half, half, sems, 3, down).start()

        def far_end(buf, size, sems):
            half = size // 2
            far_copy(buf, seg_far, 0, half, sems, 2, up).wait_recv()
            far_copy(buf, seg_far, half, half, sems, 3, down).wait_recv()
            far_copy(buf, seg, 0, size, sems, 0, up).wait_send()
            far_copy(buf, seg, 0, size, sems, 1, down).wait_send()
            far_copy(buf, seg_down, 0, half, sems, 2, up).wait_send()
            far_copy(buf, seg_up, half, half, sems, 3, down).wait_send()

        def near_copy(src, dst, to, source, sems, size):
            return pltpu.make_async_remote_copy(
                src_ref=src.at[to, pl.ds(0, size), :],
                dst_ref=dst.at[source, pl.ds(0, size), :],
                send_sem=sems[0].at[to],
                recv_sem=sems[1].at[source],
                device_id={"ka": base + to},
                device_id_type=MESH,
            )

        def at_turn(turn):
            return lax.rem(
                pos + near + near // 2 + (turn + 1) // 2 * (1 - 2 * lax.rem(turn, 2)), near
            )

        def near_start(src, dst, sems, size):
            for turn in range(near - 1):
                off = near // 2 + (turn + 1) // 2 * (1 - 2 * (turn % 2))
                near_copy(src, dst, peer(off), pos, sems, size).start()

        s_sems, p_sems = (ss_sem, sr_sem), (ps_sem, pr_sem)
        a_sems, x_sems = (as_sem, ar_sem), (xs_sem, xr_sem)
        s_rows = 4 * nf
        far_start(s_all, s_rows, s_sems)
        near_start(send_a, recv_a, a_sems, dense)
        recv_a[pos] = send_a[pos]
        orb = iota((NO, gn, 2 * LN), 0)
        which = lax.rem(iota((NO, gn, 2 * LN), 2), LN) // NO
        masks[...] = one_hot(which == orb).astype(bf16)

        e_col = dot(e2[0:1, :], jnp.ones((1, LN), f32), 0, 0)[0:rows]

        def omega_of(number, g):
            place = at_turn(per * g + number // own)
            return (2.0 * freq_of(lax.rem(number, own), place).astype(f32) + 1.0) * unit

        def left(g, _):
            om = omega_of(iota((gn, bp), 0), g)
            rec = 1.0 / (energy * energy + om * om)
            gsr[g] = -energy * rec
            gsi[g] = -om * rec
            ln = iota((rows, LN), 1)
            n64 = lax.rem(ln, gn)
            om = omega_of(n64, g)
            rec = 1.0 / (e_col * e_col + om * om)
            gr, gi = -e_col * rec, -om * rec
            first = ln < gn
            ga = jnp.where(first, gr, -gi)
            gb = jnp.where(first, gi, gr)
            for i in range(NO):
                cr, ci = pt[0, 0:rows, i : i + 1], pt[1, 0:rows, i : i + 1]
                for half, value in enumerate((ga * cr + gb * ci, gb * cr - ga * ci)):
                    th, tl = split(value)
                    for part_k, piece in enumerate((th, th, tl)):
                        at = LN * (NO * part_k + i)
                        lcat[g, rows * half : rows * half + rows, at : at + LN] = piece
            return 0

        lax.fori_loop(0, groups // 2, left, 0)
        far_relay(s_all, s_rows, s_sems)
        lax.fori_loop(groups // 2, groups, left, 0)

        sel = one_hot(
            (iota((NO * JP, LN), 1) == NO * (iota((NO * JP, LN), 0) // JP) + lax.rem(iota((NO * JP, LN), 0), JP))
            & (lax.rem(iota((NO * JP, LN), 0), JP) < NO)
        )

        def arrive(dst, sems, source, size):
            @pl.when(source != pos)
            def _():
                near_copy(dst, dst, source, source, sems, size).wait_recv()

        def wait_all(dst, sems, size):
            def one(source, _):
                arrive(dst, sems, source, size)
                return 0

            lax.fori_loop(0, near, one, 0)

        def sent_all(src, sems, size):
            def one(off, _):
                near_copy(src, src, peer(off), pos, sems, size).wait_send()
                return 0

            lax.fori_loop(1, near, one, 0)

        def cube(x):
            return x.reshape(NO, JP, batch)

        def flat(x):
            return x.reshape(NO * JP, batch)

        sr = iota((NO * JP, LN), 0)
        sc = iota((NO * JP, LN), 1)
        to_cube = one_hot(
            (dense * (sc // cut) + lax.rem(sc, cut) == NO * (sr // JP) + lax.rem(sr, JP))
            & (lax.rem(sr, JP) < NO)
            & (lax.rem(sc, cut) < dense)
        )
        eighth = iota((cut, LN), 1) // own

        def gathered(c):
            lines = []
            for q in range(4):
                halves = []
                for far_k in range(near // 8):
                    block = None
                    for k in range(8):
                        piece = recv_a[8 * far_k + k]
                        turn = (own * k - cut * q - own * c) % LN
                        piece = pltpu.roll(piece, turn, 1) if turn else piece
                        block = piece if block is None else jnp.where(eighth == k, piece, block)
                    halves.append(block)
                lines.append(jnp.concatenate(halves, axis=1))
            return cube(dot(to_cube, jnp.concatenate(lines, axis=0), 1, 0))

        wait_all(recv_a, a_sems, dense)
        ainv_r, ainv_i = invert(gathered(0), gathered(1))

        far_end(s_all, s_rows, s_sems)
        s_flat = dot(sel, s_all[...].reshape(SEGS * s_rows, LN), 1, 1)
        at_row = iota((SEGS * s_rows, batch), 0)
        slot = lax.rem(iota((SEGS * s_rows, batch), 1), own)

        def spread(kind, c):
            hit = (at_row // s_rows == slot // nf) & (
                lax.rem(at_row, s_rows) == 2 * nf * kind + nf * c + lax.rem(slot, nf)
            )
            return dot(s_flat, one_hot(hit), 1, 0)

        sg_r, sg_i = spread(0, 0), spread(0, 1)
        im_r, im_i = spread(1, 0), spread(1, 1)
        gorb = invert(ainv_r - cube(sg_r), ainv_i - cube(sg_i))
        pick = one_hot(lax.rem(iota((own, batch), 1), own) == iota((own, batch), 0))
        sums = [dot(dot(pick, flat(x), 1, 1), sel, 1, 0) for x in gorb]
        part[seg, 0:own, :] = sums[0]
        part[seg, own : 2 * own, :] = sums[1]
        far = lax.rem(me + 2 * near, devices)
        far_copy(part, seg, 0, cut, p_sems, 2, far).start()
        far_start(part, cut, p_sems)
        sent_all(send_a, a_sems, dense)
        far_copy(part, seg_down, 0, cut, p_sems, 0, up).wait_recv()
        far_copy(part, seg_up, 0, cut, p_sems, 1, down).wait_recv()
        far_copy(part, seg_far, 0, cut, p_sems, 2, far).wait_recv()
        far_copy(part, seg, 0, cut, p_sems, 0, up).wait_send()
        far_copy(part, seg, 0, cut, p_sems, 1, down).wait_send()
        far_copy(part, seg, 0, cut, p_sems, 2, far).wait_send()
        total = (part[0] + part[1] + part[2] + part[3]) * (1.0 / devices)
        t_flat = dot(sel, total, 1, 1)
        t_row = iota((2 * own, batch), 0)
        t_slot = lax.rem(iota((2 * own, batch), 1), own)
        loc = [cube(dot(t_flat, one_hot(t_row == t_slot + own * c), 1, 0)) for c in range(2)]
        linv_r, linv_i = invert(*loc)
        d_r, d_i = flat(linv_r) - im_r, flat(linv_i) - im_i
        q0, q1 = iota((NO * JP, NO * JP), 0), iota((NO * JP, NO * JP), 1)
        same = one_hot(q0 == q1)
        turned = one_hot((q0 // JP == lax.rem(q1, JP)) & (lax.rem(q0, JP) == q1 // JP))
        new_r = sg_r + dot(0.5 * (same + turned), d_r, 1, 0)
        new_i = sg_i + dot(0.5 * (same - turned), d_i, 1, 0)

        own_row = iota((8, batch), 0)
        own_lane = iota((8, batch), 1)
        last = one_hot((own_lane == own - 1) & (own_row == 0))
        last_r = dot(dot(last, new_r, 1, 1), sel, 1, 0)
        last_i = dot(dot(last, new_i, 1, 1), sel, 1, 0)
        h_src[...] = last_r + pltpu.roll(last_i, 1, 0)

        def h_copy(off, sem):
            return pltpu.make_async_remote_copy(
                src_ref=h_src,
                dst_ref=h_dst,
                send_sem=hs_sem.at[sem],
                recv_sem=hr_sem,
                device_id={"ka": base + peer(off)},
                device_id_type=MESH,
            )

        gnew = invert(ainv_r - cube(new_r), ainv_i - cube(new_i))
        sn = cube(new_r), cube(new_i)
        half = cmul(*sn, *gnew)
        full = cmul(*half, *sn)
        for c in range(2):
            x = dot(flat(sn[c] + full[c]), sel, 0, 0)
            send_x[:, c * own : (c + 1) * own, :] = x.reshape(near, own, LN)
        @pl.when(pos == near - 1)
        def _():
            for off in range(1, near):
                h_copy(off, off).start()
            keep = pltpu.make_async_copy(h_src, h_dst, loc_sem)
            keep.start()
            keep.wait()

        near_start(send_x, recv_x, x_sems, cut)
        recv_x[pos] = send_x[pos]

        mine_hit = (own_row < nf) & (own_lane == nf * seg + own_row)
        mine = one_hot(mine_hit)
        for c, value in enumerate((new_r, new_i)):
            lines = dot(dot(mine, value, 1, 1), sel, 1, 0)
            for i in range(NO):
                place = one_hot(iota((NO, LN), 1) == NO * i + iota((NO, LN), 0))
                out_ref[c, i] = dot(lines, place, 1, 1)[0:nf]

        pjt_r, pjt_i = dot(oh_j, pr, 0, 0), dot(oh_j, pi, 0, 0)
        wide = jnp.concatenate(
            [
                jnp.concatenate([pjt_r, -pjt_i], axis=0),
                jnp.concatenate([pjt_i, pjt_r], axis=0),
            ],
            axis=1,
        )
        w_high, w_low = split(wide)
        for k, piece in enumerate((w_high, w_low, w_high)):
            wcat[2 * LN * k : 2 * LN * k + 2 * LN, :] = piece
        cacc[...] = jnp.zeros_like(cacc)

        def offset(turn):
            return near // 2 + (turn + 1) // 2 * (1 - 2 * (turn % 2))

        def wait_group(g):
            for turn in range(per * g, per * g + per):
                if offset(turn) % near:
                    source = peer(offset(turn))
                    near_copy(recv_x, recv_x, source, source, x_sems, cut).wait_recv()

        def right(g):
            blocks = [recv_x[peer(offset(turn))] for turn in range(per * g, per * g + per)]
            x = jnp.concatenate(
                [
                    jnp.concatenate([b[c * own : (c + 1) * own] for b in blocks], axis=0)
                    for c in range(2)
                ],
                axis=1,
            )
            xh, xl = split(x)
            xh = (xh[None] * masks[...]).reshape(NO * gn, 2 * LN)
            xl = (xl[None] * masks[...]).reshape(NO * gn, 2 * LN)
            mixed = bdot(jnp.concatenate([xh, xh, xl], axis=1), wcat[...])
            gr, gi = gsr[g], gsi[g]
            slot_r = g % 2
            for i in range(NO):
                a, b = mixed[gn * i : gn * i + gn, 0:bp], mixed[gn * i : gn * i + gn, bp : 2 * bp]
                for c, value in enumerate((a * gr - b * gi, a * gi + b * gr)):
                    th, tl = split(value)
                    for k, piece in enumerate((th, tl, th)):
                        at = NO * LN * k + LN * i + gn * c
                        rcat[slot_r, at : at + gn, :] = piece

        def total_of(g):
            cacc[...] += bdot(lcat[g], rcat[g % 2])

        def tail():
            def square(line):
                wide = jnp.broadcast_to(line, (JP, LN))
                return dot(wide * oh_i, oh_j, 1, 1), dot(wide * oh_j, oh_i, 1, 1)

            m_r, mt_r = square(h_dst[0:1, :])
            m_i, mt_i = square(h_dst[1:2, :])
            h_r, h_i = 0.5 * (m_r + mt_r), 0.5 * (m_i - mt_i)
            hp_r = dot(h_r, pr, 1, 0) - dot(h_i, pi, 1, 0)
            hp_i = dot(h_r, pi, 1, 0) + dot(h_i, pr, 1, 0)
            ptr, pti = pt[0], pt[1]
            quad_r = dot(ptr, hp_r, 1, 0) + dot(pti, hp_i, 1, 0)
            quad_i = dot(ptr, hp_i, 1, 0) - dot(pti, hp_r, 1, 0)
            return quad_r, quad_i

        for g in range(groups):
            wait_group(g)
            if g == 1:
                @pl.when(pos != near - 1)
                def _():
                    h_copy(1, 0).wait_recv()

                quad_r, quad_i = tail()
            right(g)
            if g:
                total_of(g - 1)
        total_of(groups - 1)
        c_r = jnp.concatenate([cacc[0:bands, :], jnp.zeros((bp - bands, bp), f32)], axis=0)
        c_i = jnp.concatenate([cacc[rows : rows + bands, :], jnp.zeros((bp - bands, bp), f32)], axis=0)
        scale = 1.0 / inverse_temp
        d0 = (c_r + c_r.T) * scale - weight * quad_r
        d1 = (c_i - c_i.T) * scale - weight * quad_i
        dens_ref[0, 0] = d0[0:bands, 0:bands]
        dens_ref[0, 1] = d1[0:bands, 0:bands]

        sent_all(send_x, x_sems, cut)

        @pl.when(pos == near - 1)
        def _():
            for off in range(1, near):
                h_copy(off, off).wait_send()

    dma = pltpu.SemaphoreType.DMA
    return pl.pallas_call(
        kernel,
        out_shape=(
            jax.ShapeDtypeStruct((1, 2, bands, bands), f32),
            jax.ShapeDtypeStruct((2, NO, nf, NO), f32),
        ),
        in_specs=[pl.BlockSpec(memory_space=pltpu.HBM)] * 5,
        out_specs=(pl.BlockSpec(memory_space=pltpu.VMEM),) * 2,
        scratch_shapes=[
            pltpu.VMEM((1, 2), jnp.int32),
            pltpu.VMEM((1, bands), f32),
            pltpu.VMEM((1, NO, 2, bands), f32),
            pltpu.VMEM((2, NO, nf, NO), f32),
            pltpu.VMEM((2, NO, nf, NO), f32),
            pltpu.VMEM((2, JP, bp), f32),
            pltpu.VMEM((2, bp, JP), f32),
            pltpu.VMEM((8, bp), f32),
            pltpu.VMEM((NO, 4 * nf, LN), f32),
            pltpu.VMEM((groups, gn, bp), f32),
            pltpu.VMEM((groups, gn, bp), f32),
            pltpu.VMEM((NO, gn, 2 * LN), bf16),
            pltpu.VMEM((SEGS, 4 * nf, LN), f32),
            pltpu.VMEM((SEGS, 2 * own, LN), f32),
            pltpu.VMEM((near, 2 * own, LN), f32),
            pltpu.VMEM((near, 2 * own, LN), f32),
            pltpu.VMEM((near, 2 * own, LN), f32),
            pltpu.VMEM((near, 2 * own, LN), f32),
            pltpu.VMEM((8, LN), f32),
            pltpu.VMEM((8, LN), f32),
            pltpu.VMEM((groups, 2 * rows, 3 * NO * LN), bf16),
            pltpu.VMEM((2, 3 * NO * LN, bp), bf16),
            pltpu.VMEM((6 * LN, 2 * bp), bf16),
            pltpu.VMEM((2 * rows, bp), f32),
            dma((near,)), dma((near,)), dma((near,)), dma((near,)),
            dma((4,)), dma((4,)), dma((4,)), dma((4,)),
            dma((near,)), dma, dma, dma((5,)),
        ],
        compiler_params=pltpu.CompilerParams(
            collective_id=0, has_side_effects=True, vmem_limit_bytes=67043328
        ),
        name="charge_update",
    )


def solution(mesh):
    devices = mesh.shape["ka"]

    def local(energies, proj, window, sigma, impurity_inverse):
        call = build(devices, sigma.shape[3], energies.shape[1])
        density, new = call(
            window,
            energies,
            jnp.swapaxes(proj, 1, 2),
            jnp.swapaxes(sigma, 2, 3),
            jnp.swapaxes(impurity_inverse, 2, 3),
        )
        return density, jnp.swapaxes(new, 2, 3)

    both = ("parts", "ka")
    in_specs = (
        P(both, None),
        P(both, None, None, None),
        P(both, None),
        P("parts", None, None, "ka"),
        P("parts", None, None, "ka"),
    )
    out_specs = (P(both, None, None, None), P("parts", None, None, "ka"))
    return jax.shard_map(local, mesh=mesh, in_specs=in_specs, out_specs=out_specs, check_vma=False)
```
